32 devices in a mesh: rows: 8 (over z, x), width: 4 (over y, core).
Axes of the slice: x: 2, y: 2, z: 4, core: 2. Of those that a mesh axis runs over, the one named last changes fastest.
Arguments:
- weight_gate: float32 [2560, 9728], P('rows', 'width'), may hold values from -0.15625 to 0.15625
- moment_gate: float32 [2560, 9728], P('rows', 'width'), may hold values from -6 to 6
- square_gate: float32 [2560, 9728], P('rows', 'width'), may hold values from 0.1 to 10
- weight_up: float32 [2560, 9728], P('rows', 'width'), may hold values from -0.15625 to 0.15625
- moment_up: float32 [2560, 9728], P('rows', 'width'), may hold values from -6 to 6
- square_up: float32 [2560, 9728], P('rows', 'width'), may hold values from 0.1 to 10
- norm_gain: float32 [2560], P('rows'), may hold values from 0.25 to 1.75
Outputs:
- ready_gate: bfloat16 [2560, 9728], P(None, 'width')
- ready_up: bfloat16 [2560, 9728], P(None, 'width')
- column_gate: float32 [9728], P('width')
- column_up: float32 [9728], P('width')
The draws below stay inside these ranges and needn't reach their ends.
All inputs are finite; a program needn't handle non-finite values.
Results may differ from the reference program's by a relative error of at most 0.0004.
Values may be sent and summed in bfloat16 or wider, within the bound.
A program may use at most 128 MiB of HBM per device.

```python
import math
import jax
import jax.numpy as jnp
from jax import lax

D_MODEL = 2560
D_INNER = 9728


def with_spikes(values, rng, source, target, blocks, factor):
    def block_of(axis_at):
        return (jnp.arange(values.shape[axis_at]) // (values.shape[axis_at] // blocks)).reshape((-1,) + (1,) * (values.ndim - 1 - axis_at))

    one_side = jax.random.permutation(rng, blocks)[block_of(target)]
    second = (block_of(target) + blocks // 2) % blocks
    return jnp.where((block_of(source) == one_side) | (block_of(source) == second), factor * values, values)


def block_levels(rng, extent, pieces, smallest, top_value):
    loudness, own = 1.0, jax.random.fold_in(rng, 6)
    for dim, blocks in pieces:
        heights = jnp.exp(jax.random.uniform(jax.random.fold_in(own, dim), (blocks,), jnp.float32, smallest / len(pieces), top_value / len(pieces)))
        loudness = loudness * jnp.repeat(heights, extent[dim] // blocks).reshape([-1 if axis == dim else 1 for axis in range(len(extent))])
    return loudness


def normal_values(own_key, shape, scale, limit, split=(), held_as=jnp.bfloat16):
    array = scale * jax.random.normal(own_key, shape, jnp.float32)
    if split:
        array = array * block_levels(own_key, shape, split, -0.22, 0.18)
    return jnp.clip(array, -limit, limit).astype(held_as)


def noise_with(rng, dims, spread, most, shards, heavy, dtype=jnp.bfloat16):
    entries = spread * jax.random.normal(rng, dims, jnp.float32)
    if shards:
        entries = entries * block_levels(rng, dims, shards, -0.22, 0.18)
    return jnp.clip(with_spikes(entries, jax.random.fold_in(rng, 3), *heavy), -most, most).astype(dtype)


def setup_inputs(seed: int = 0) -> dict:
    arg_keys = jax.random.split(jax.random.key(seed), 8)
    return {
        "weight_gate": noise_with(arg_keys[0], (D_MODEL, D_INNER), D_MODEL ** -0.5, 0.15625, ((0, 8), (1, 4)), (0, 1, 8, 2.0), jnp.float32),
        "moment_gate": normal_values(arg_keys[1], (D_MODEL, D_INNER), 1.0, 6.0, ((0, 8), (1, 4)), jnp.float32),
        "square_gate": jnp.clip(jnp.exp(math.log(10.0) - 4.6051702 * jax.random.uniform(arg_keys[2], (D_MODEL, D_INNER), jnp.float32) ** block_levels(arg_keys[2], (D_MODEL, D_INNER), ((0, 8), (1, 4)), -0.2, 0.2)), 0.1, 10.0),
        "weight_up": noise_with(arg_keys[3], (D_MODEL, D_INNER), D_MODEL ** -0.5, 0.15625, ((0, 8), (1, 4)), (0, 1, 8, 2.0), jnp.float32),
        "moment_up": normal_values(arg_keys[4], (D_MODEL, D_INNER), 1.0, 6.0, ((0, 8), (1, 4)), jnp.float32),
        "square_up": jnp.clip(jnp.exp(math.log(10.0) - 4.6051702 * jax.random.uniform(arg_keys[5], (D_MODEL, D_INNER), jnp.float32) ** block_levels(arg_keys[5], (D_MODEL, D_INNER), ((0, 8), (1, 4)), -0.2, 0.2)), 0.1, 10.0),
        "norm_gain": jnp.clip(1.0 + 0.15 * jax.random.normal(arg_keys[6], (D_MODEL,), jnp.float32), 0.25, 1.75),
    }


learn_rate = 0.02
decay_rate = 0.1
tiny_value = 1e-08

def reference(weight_gate, moment_gate, square_gate, weight_up, moment_up, square_up, norm_gain):
    latest_gate = weight_gate - learn_rate * (moment_gate / (jnp.sqrt(square_gate) + tiny_value) + decay_rate * weight_gate)
    latest_up = weight_up - learn_rate * (moment_up / (jnp.sqrt(square_up) + tiny_value) + decay_rate * weight_up)
    latest_gained_gate = latest_gate * norm_gain[:, None]
    latest_gained_up = latest_up * norm_gain[:, None]
    column_gate = jnp.sqrt(lax.optimization_barrier(jnp.sum(latest_gained_gate * latest_gained_gate, axis=0)))
    ready_gate = (latest_gained_gate / column_gate).astype(jnp.bfloat16)
    column_up = jnp.sqrt(lax.optimization_barrier(jnp.sum(latest_gained_up * latest_gained_up, axis=0)))
    ready_up = (latest_gained_up / column_up).astype(jnp.bfloat16)
    return (ready_gate, ready_up, column_gate, column_up)
```

```python
import functools

import jax
import jax.numpy as jnp
from jax import lax
from jax.experimental import pallas as pl
from jax.experimental.pallas import tpu as pltpu
from jax.sharding import PartitionSpec as P

learn_rate = 0.02
decay_rate = 0.1
tiny_value = 1e-08
lanes = 128
block_rows = 16
MESH = pl.DeviceIdType.MESH


def column_cuts(columns):
    tiles = columns // lanes
    first = max(1, tiles // 9)
    rest = tiles - first
    sizes = [first] + [rest // 3 + (1 if i < rest % 3 else 0) for i in range(3)]
    cuts, at = [], 0
    for size in sizes:
        if size:
            cuts.append((at * lanes, size * lanes))
        at += size
    return cuts


def gather_kernel(
    n, gain_ref, wg, mg, sg, wu, mu, su, out_gate, out_up, col_gate, col_up,
    values, moments, squares, ready, parts, in_sem, own_sem, part_send, part_recv, send_sem, recv_sem,
):
    me = lax.axis_index("rows")
    w = lax.axis_index("width")
    length = n // 2
    place, side = me // 2, me % 2
    mate = place + 1 - 2 * (place % 2)
    rows, columns = wg.shape
    cuts = column_cuts(columns)
    half = len(cuts)
    chunks = [(t, at, size) for t in range(2) for at, size in cuts]
    sources = ((wg, mg, sg), (wu, mu, su))
    outs = (out_gate, out_up)
    cols = (col_gate, col_up)

    def fetch(k):
        t, at, size = chunks[k]
        return [
            pltpu.make_async_copy(src.at[:, pl.ds(at, size)], dst.at[t, :, pl.ds(at, size)], in_sem.at[i, k])
            for i, (src, dst) in enumerate(zip(sources[t], (values, moments, squares)))
        ]

    for k in range(len(chunks)):
        for copy in fetch(k):
            copy.start()

    barrier = pltpu.get_barrier_semaphore()

    def greet(i, carry):
        peer = lax.rem(me + i, n)
        pl.semaphore_signal(barrier, inc=1, device_id=(peer, w), device_id_type=MESH)
        return carry

    lax.fori_loop(1, n, greet, 0)

    def part_copy(k, peer):
        t, at, size = chunks[k]
        here = parts.at[me, t, :, pl.ds(at, size)]
        return pltpu.make_async_remote_copy(
            src_ref=here, dst_ref=here, send_sem=part_send.at[k], recv_sem=part_recv.at[k],
            device_id=(peer, w), device_id_type=MESH,
        )

    def compute(k):
        t, at, size = chunks[k]
        for copy in fetch(k):
            copy.wait()

        def step(b, total):
            here = pl.ds(pl.multiple_of(b * block_rows, block_rows), block_rows)
            there = pl.ds(at, size)
            weight = values[t, here, there]
            latest = weight - learn_rate * (
                moments[t, here, there] / (jnp.sqrt(squares[t, here, there]) + tiny_value) + decay_rate * weight
            )
            gain = jnp.concatenate([gain_ref[here, :]] * (size // lanes), axis=1)
            gained = latest * gain
            values[t, here, there] = gained
            squared = gained * gained
            for r in range(0, block_rows, 8):
                total = total + squared[r : r + 8]
            return total

        total = lax.fori_loop(0, rows // block_rows, step, jnp.zeros((8, size), jnp.float32))
        parts[me, t, :, pl.ds(at, size)] = jnp.sum(total, axis=0, keepdims=True)

    def share_parts(k):
        def send(i, carry):
            part_copy(k, lax.rem(me + i, n)).start()
            return carry

        lax.fori_loop(1, n, send, 0)

    def part_bytes(k, sem):
        t, at, size = chunks[k]
        refs = parts.at[pl.ds(0, n - 1), t, :, pl.ds(at, size)]
        return pltpu.make_async_copy(refs, refs, sem)

    def block(share, k):
        t, at, size = chunks[k]
        start = pl.multiple_of(share * rows, rows)
        return outs[t].at[pl.ds(start, rows), pl.ds(at, size)]

    own_slot = 0

    def own(k):
        t, at, size = chunks[k]
        return ready.at[t, :, pl.ds(at, size)]

    def keep(k):
        return pltpu.make_async_copy(own(k), block(me, k), own_sem.at[k])

    def push(link, slot, share, k):
        there = ((place - 1) * 2 + side, (place + 1) * 2 + side, place * 2 + 1 - side)[link]
        here = block(share, k)
        return pltpu.make_async_remote_copy(
            src_ref=own(k) if slot is own_slot else here, dst_ref=here,
            send_sem=send_sem.at[link, slot, k], recv_sem=recv_sem.at[share, k],
            device_id=(there, w), device_id_type=MESH,
        )

    def arrived(share, k):
        here = block(share, k)
        pltpu.make_async_copy(here, here, recv_sem.at[share, k]).wait()

    def finish(k):
        t, at, size = chunks[k]
        part_bytes(k, part_recv.at[k]).wait()
        total = parts[0, t, :, pl.ds(at, size)]
        for i in range(1, n):
            total = total + parts[i, t, :, pl.ds(at, size)]
        scale = jnp.sqrt(total)
        cols[t][:, pl.ds(at, size)] = scale

        def step(b, carry):
            here = pl.ds(pl.multiple_of(b * block_rows, block_rows), block_rows)
            ready[t, here, pl.ds(at, size)] = (values[t, here, pl.ds(at, size)] / scale).astype(jnp.bfloat16)
            return carry

        lax.fori_loop(0, rows // block_rows, step, 0)

    def send_own(k):
        @pl.when(place > 0)
        def _():
            push(0, 0, me, k).start()

        @pl.when(place < length - 1)
        def _():
            push(1, 0, me, k).start()

        push(2, 0, me, k).start()
        keep(k).start()

    compute(0)
    pl.semaphore_wait(barrier, n - 1)
    share_parts(0)
    for k in range(len(chunks)):
        if k + 1 < len(chunks):
            compute(k + 1)
            share_parts(k + 1)
        finish(k)
        send_own(k)

    def spread(d, carry):
        for k in range(len(chunks)):
            @pl.when(place + d < length)
            def _():
                share = (place + d) * 2 + side
                arrived(share, k)

                @pl.when(place > 0)
                def _():
                    push(0, d, share, k).start()

                if k < half:
                    push(2, d, share, k).start()
                else:
                    @pl.when(place + d != mate)
                    def _():
                        push(2, d, share, k).start()

            @pl.when(place - d >= 0)
            def _():
                share = (place - d) * 2 + side
                arrived(share, k)

                @pl.when(place < length - 1)
                def _():
                    push(1, d, share, k).start()

                if k < half:
                    push(2, length + d, share, k).start()
                else:
                    @pl.when(place - d != mate)
                    def _():
                        push(2, length + d, share, k).start()

        return carry

    def extra(action):
        share = place * 2 + 1 - side
        for k in range(half, len(chunks)):
            if action == "start":
                arrived(share, k)

            @pl.when(mate < place)
            def _():
                copy = push(0, length, share, k)
                copy.start() if action == "start" else copy.wait_send()

            @pl.when(mate > place)
            def _():
                copy = push(1, length, share, k)
                copy.start() if action == "start" else copy.wait_send()

    middle = max(1, length // 2) + 1
    lax.fori_loop(1, middle, spread, 0)
    extra("start")
    lax.fori_loop(middle, length, spread, 0)

    def collect(q, carry):
        share = q * 2 + 1 - side
        for k in range(len(chunks)):
            if k < half:
                arrived(share, k)
            else:
                @pl.when(q != place)
                def _():
                    arrived(share, k)
        return carry

    lax.fori_loop(0, length, collect, 0)

    for k in range(len(chunks)):
        part_bytes(k, part_send.at[k]).wait()
        keep(k).wait()

        @pl.when(place > 0)
        def _():
            push(0, 0, me, k).wait_send()

        @pl.when(place < length - 1)
        def _():
            push(1, 0, me, k).wait_send()

        push(2, 0, me, k).wait_send()
    extra("wait")

    def drain(d, carry):
        for k in range(len(chunks)):
            @pl.when(place + d < length)
            def _():
                share = (place + d) * 2 + side

                @pl.when(place > 0)
                def _():
                    push(0, d, share, k).wait_send()

                if k < half:
                    push(2, d, share, k).wait_send()
                else:
                    @pl.when(place + d != mate)
                    def _():
                        push(2, d, share, k).wait_send()

            @pl.when(place - d >= 0)
            def _():
                share = (place - d) * 2 + side

                @pl.when(place < length - 1)
                def _():
                    push(1, d, share, k).wait_send()

                if k < half:
                    push(2, length + d, share, k).wait_send()
                else:
                    @pl.when(place - d != mate)
                    def _():
                        push(2, length + d, share, k).wait_send()

        return carry

    lax.fori_loop(1, length, drain, 0)


def per_device(n, weight_gate, moment_gate, square_gate, weight_up, moment_up, square_up, norm_gain):
    rows, columns = weight_gate.shape
    gain = jnp.broadcast_to(norm_gain[:, None], (rows, lanes))
    count = 2 * len(column_cuts(columns))
    vmem = pl.BlockSpec(memory_space=pltpu.VMEM)
    hbm = pl.BlockSpec(memory_space=pltpu.HBM)
    scratch_bytes = 7 * rows * columns * 4
    ready_gate, ready_up, column_gate, column_up = pl.pallas_call(
        functools.partial(gather_kernel, n),
        out_shape=(
            jax.ShapeDtypeStruct((n * rows, columns), jnp.bfloat16),
            jax.ShapeDtypeStruct((n * rows, columns), jnp.bfloat16),
            jax.ShapeDtypeStruct((1, columns), jnp.float32),
            jax.ShapeDtypeStruct((1, columns), jnp.float32),
        ),
        in_specs=[vmem] + [hbm] * 6,
        out_specs=(hbm, hbm, vmem, vmem),
        scratch_shapes=[
            pltpu.VMEM((2, rows, columns), jnp.float32),
            pltpu.VMEM((2, rows, columns), jnp.float32),
            pltpu.VMEM((2, rows, columns), jnp.float32),
            pltpu.VMEM((2, rows, columns), jnp.bfloat16),
            pltpu.VMEM((n, 2, 1, columns), jnp.float32),
            pltpu.SemaphoreType.DMA((3, count)),
            pltpu.SemaphoreType.DMA((count,)),
            pltpu.SemaphoreType.DMA((count,)),
            pltpu.SemaphoreType.DMA((count,)),
            pltpu.SemaphoreType.DMA((3, n, count)),
            pltpu.SemaphoreType.DMA((n, count)),
        ],
        compiler_params=pltpu.CompilerParams(
            collective_id=0, has_side_effects=True, vmem_limit_bytes=scratch_bytes + 8 * 2**20
        ),
        name="step_and_gather",
    )(gain, weight_gate, moment_gate, square_gate, weight_up, moment_up, square_up)
    return ready_gate, ready_up, column_gate.reshape(columns), column_up.reshape(columns)


def solution(mesh):
    split = P("rows", "width")
    return jax.shard_map(
        functools.partial(per_device, mesh.shape["rows"]),
        mesh=mesh,
        in_specs=(split,) * 6 + (P("rows"),),
        out_specs=(P(None, "width"), P(None, "width"), P("width"), P("width")),
        check_vma=False,
    )
```

```python
import functools

import jax
import jax.numpy as jnp
from jax import lax
from jax.experimental import pallas as pl
from jax.experimental.pallas import tpu as pltpu
from jax.sharding import PartitionSpec as P

learn_rate = 0.02
decay_rate = 0.1
tiny_value = 1e-08
lanes = 128
vmem_bytes = 67043328
block_rows = 16
MESH = pl.DeviceIdType.MESH


def column_cuts(columns):
    tiles = columns // lanes
    first = max(1, tiles // 9)
    rest = tiles - first
    sizes = [first] + [rest // 3 + (1 if i < rest % 3 else 0) for i in range(3)]
    cuts, at = [], 0
    for size in sizes:
        if size:
            cuts.append((at * lanes, size * lanes))
        at += size
    return cuts


def gather_kernel(
    n, gain_ref, wg, mg, sg, wu, mu, su, out_gate, out_up, col_gate, col_up,
    values, moments, squares, parts, in_sem, part_send, part_recv, send_sem, recv_sem,
):
    me = lax.axis_index("rows")
    w = lax.axis_index("width")
    length = n // 2
    place, side = me // 2, me % 2
    mate = place + 1 - 2 * (place % 2)
    rows, columns = wg.shape
    cuts = column_cuts(columns)
    half = len(cuts)
    chunks = [(t, at, size) for t in range(2) for at, size in cuts]
    sources = ((wg, mg, sg), (wu, mu, su))
    outs = (out_gate, out_up)
    cols = (col_gate, col_up)

    def fetch(k):
        t, at, size = chunks[k]
        return [
            pltpu.make_async_copy(src.at[:, pl.ds(at, size)], dst.at[t, :, pl.ds(at, size)], in_sem.at[i, k])
            for i, (src, dst) in enumerate(zip(sources[t], (values, moments, squares)))
        ]

    for k in range(len(chunks)):
        for copy in fetch(k):
            copy.start()

    barrier = pltpu.get_barrier_semaphore()

    def greet(i, carry):
        peer = lax.rem(me + i, n)
        pl.semaphore_signal(barrier, inc=1, device_id=(peer, w), device_id_type=MESH)
        return carry

    lax.fori_loop(1, n, greet, 0)

    def part_copy(k, peer):
        t, at, size = chunks[k]
        here = parts.at[me, t, :, pl.ds(at, size)]
        return pltpu.make_async_remote_copy(
            src_ref=here, dst_ref=here, send_sem=part_send.at[k], recv_sem=part_recv.at[k],
            device_id=(peer, w), device_id_type=MESH,
        )

    def compute(k):
        t, at, size = chunks[k]
        for copy in fetch(k):
            copy.wait()

        def step(b, total):
            here = pl.ds(pl.multiple_of(b * block_rows, block_rows), block_rows)
            there = pl.ds(at, size)
            weight = values[t, here, there]
            latest = weight - learn_rate * (
                moments[t, here, there] / (jnp.sqrt(squares[t, here, there]) + tiny_value) + decay_rate * weight
            )
            gain = jnp.concatenate([gain_ref[here, :]] * (size // lanes), axis=1)
            gained = latest * gain
            values[t, here, there] = gained
            squared = gained * gained
            for r in range(0, block_rows, 8):
                total = total + squared[r : r + 8]
            return total

        total = lax.fori_loop(0, rows // block_rows, step, jnp.zeros((8, size), jnp.float32))
        parts[me, t, :, pl.ds(at, size)] = jnp.sum(total, axis=0, keepdims=True)

    def share_parts(k):
        def send(i, carry):
            part_copy(k, lax.rem(me + i, n)).start()
            return carry

        lax.fori_loop(1, n, send, 0)

    def part_bytes(k, sem):
        t, at, size = chunks[k]
        refs = parts.at[pl.ds(0, n - 1), t, :, pl.ds(at, size)]
        return pltpu.make_async_copy(refs, refs, sem)

    def block(share, k):
        t, at, size = chunks[k]
        start = pl.multiple_of(share * rows, rows)
        return outs[t].at[pl.ds(start, rows), pl.ds(at, size)]

    def push(link, slot, share, k):
        there = ((place - 1) * 2 + side, (place + 1) * 2 + side, place * 2 + 1 - side)[link]
        here = block(share, k)
        return pltpu.make_async_remote_copy(
            src_ref=here, dst_ref=here,
            send_sem=send_sem.at[link, slot, k], recv_sem=recv_sem.at[share, k],
            device_id=(there, w), device_id_type=MESH,
        )

    def arrived(share, k):
        here = block(share, k)
        pltpu.make_async_copy(here, here, recv_sem.at[share, k]).wait()

    def finish(k):
        t, at, size = chunks[k]
        part_bytes(k, part_recv.at[k]).wait()
        total = parts[0, t, :, pl.ds(at, size)]
        for i in range(1, n):
            total = total + parts[i, t, :, pl.ds(at, size)]
        scale = jnp.sqrt(total)
        cols[t][:, pl.ds(at, size)] = scale

        def step(b, carry):
            here = pl.ds(pl.multiple_of(b * block_rows, block_rows), block_rows)
            there = pl.ds(pl.multiple_of(me * rows + b * block_rows, block_rows), block_rows)
            outs[t][there, pl.ds(at, size)] = (values[t, here, pl.ds(at, size)] / scale).astype(jnp.bfloat16)
            return carry

        lax.fori_loop(0, rows // block_rows, step, 0)

    def send_own(k):
        @pl.when(place > 0)
        def _():
            push(0, 0, me, k).start()

        @pl.when(place < length - 1)
        def _():
            push(1, 0, me, k).start()

        push(2, 0, me, k).start()

    compute(0)
    pl.semaphore_wait(barrier, n - 1)
    share_parts(0)
    for k in range(len(chunks)):
        if k + 1 < len(chunks):
            compute(k + 1)
            share_parts(k + 1)
        finish(k)
        send_own(k)

    def spread(d, carry):
        for k in range(len(chunks)):
            @pl.when(place + d < length)
            def _():
                share = (place + d) * 2 + side
                arrived(share, k)

                @pl.when(place > 0)
                def _():
                    push(0, d, share, k).start()

                if k < half:
                    push(2, d, share, k).start()
                else:
                    @pl.when(place + d != mate)
                    def _():
                        push(2, d, share, k).start()

            @pl.when(place - d >= 0)
            def _():
                share = (place - d) * 2 + side
                arrived(share, k)

                @pl.when(place < length - 1)
                def _():
                    push(1, d, share, k).start()

                if k < half:
                    push(2, length + d, share, k).start()
                else:
                    @pl.when(place - d != mate)
                    def _():
                        push(2, length + d, share, k).start()

        return carry

    def extra(action):
        share = place * 2 + 1 - side
        for k in range(half, len(chunks)):
            if action == "start":
                arrived(share, k)

            @pl.when(mate < place)
            def _():
                copy = push(0, length, share, k)
                copy.start() if action == "start" else copy.wait_send()

            @pl.when(mate > place)
            def _():
                copy = push(1, length, share, k)
                copy.start() if action == "start" else copy.wait_send()

    middle = max(1, length // 2) + 1
    lax.fori_loop(1, middle, spread, 0)
    extra("start")
    lax.fori_loop(middle, length, spread, 0)

    def collect(q, carry):
        share = q * 2 + 1 - side
        for k in range(len(chunks)):
            if k < half:
                arrived(share, k)
            else:
                @pl.when(q != place)
                def _():
                    arrived(share, k)
        return carry

    lax.fori_loop(0, length, collect, 0)

    for k in range(len(chunks)):
        part_bytes(k, part_send.at[k]).wait()

        @pl.when(place > 0)
        def _():
            push(0, 0, me, k).wait_send()

        @pl.when(place < length - 1)
        def _():
            push(1, 0, me, k).wait_send()

        push(2, 0, me, k).wait_send()
    extra("wait")

    def drain(d, carry):
        for k in range(len(chunks)):
            @pl.when(place + d < length)
            def _():
                share = (place + d) * 2 + side

                @pl.when(place > 0)
                def _():
                    push(0, d, share, k).wait_send()

                if k < half:
                    push(2, d, share, k).wait_send()
                else:
                    @pl.when(place + d != mate)
                    def _():
                        push(2, d, share, k).wait_send()

            @pl.when(place - d >= 0)
            def _():
                share = (place - d) * 2 + side

                @pl.when(place < length - 1)
                def _():
                    push(1, d, share, k).wait_send()

                if k < half:
                    push(2, length + d, share, k).wait_send()
                else:
                    @pl.when(place - d != mate)
                    def _():
                        push(2, length + d, share, k).wait_send()

        return carry

    lax.fori_loop(1, length, drain, 0)


def write_kernel(pieces, gate, up, out_gate, out_up, sem):
    step = gate.shape[0] // pieces
    copies = [
        pltpu.make_async_copy(src.at[pl.ds(i * step, step)], dst.at[pl.ds(i * step, step)], sem.at[t, i])
        for i in range(pieces)
        for t, (src, dst) in enumerate(((gate, out_gate), (up, out_up)))
    ]
    for copy in copies:
        copy.start()
    for copy in copies:
        copy.wait()


def write_out(pieces, gate, up):
    vmem = pl.BlockSpec(memory_space=pltpu.VMEM)
    hbm = pl.BlockSpec(memory_space=pltpu.HBM)
    return pl.pallas_call(
        functools.partial(write_kernel, pieces),
        out_shape=[jax.ShapeDtypeStruct(a.shape, a.dtype) for a in (gate, up)],
        in_specs=[vmem, vmem],
        out_specs=[hbm, hbm],
        scratch_shapes=[pltpu.SemaphoreType.DMA((2, pieces))],
        compiler_params=pltpu.CompilerParams(vmem_limit_bytes=2**20),
        name="write_out",
    )(gate, up)


def per_device(n, weight_gate, moment_gate, square_gate, weight_up, moment_up, square_up, norm_gain):
    rows, columns = weight_gate.shape
    gain = jnp.broadcast_to(norm_gain[:, None], (rows, lanes))
    count = 2 * len(column_cuts(columns))
    vmem = pl.BlockSpec(memory_space=pltpu.VMEM)
    hbm = pl.BlockSpec(memory_space=pltpu.HBM)
    room = vmem_bytes - 2 * n * rows * columns * 2 - 3 * 2**19
    ready_gate, ready_up, column_gate, column_up = pl.pallas_call(
        functools.partial(gather_kernel, n),
        out_shape=(
            pltpu.VMEM((n * rows, columns), jnp.bfloat16),
            pltpu.VMEM((n * rows, columns), jnp.bfloat16),
            jax.ShapeDtypeStruct((1, columns), jnp.float32),
            jax.ShapeDtypeStruct((1, columns), jnp.float32),
        ),
        in_specs=[vmem] + [hbm] * 6,
        out_specs=(vmem, vmem, vmem, vmem),
        scratch_shapes=[
            pltpu.VMEM((2, rows, columns), jnp.float32),
            pltpu.VMEM((2, rows, columns), jnp.float32),
            pltpu.VMEM((2, rows, columns), jnp.float32),
            pltpu.VMEM((n, 2, 1, columns), jnp.float32),
            pltpu.SemaphoreType.DMA((3, count)),
            pltpu.SemaphoreType.DMA((count,)),
            pltpu.SemaphoreType.DMA((count,)),
            pltpu.SemaphoreType.DMA((3, n, count)),
            pltpu.SemaphoreType.DMA((n, count)),
        ],
        compiler_params=pltpu.CompilerParams(
            collective_id=0, has_side_effects=True, vmem_limit_bytes=room
        ),
        name="step_and_gather",
    )(gain, weight_gate, moment_gate, square_gate, weight_up, moment_up, square_up)
    ready_gate, ready_up = write_out(n, ready_gate, ready_up)
    return ready_gate, ready_up, column_gate.reshape(columns), column_up.reshape(columns)


def solution(mesh):
    split = P("rows", "width")
    return jax.shard_map(
        functools.partial(per_device, mesh.shape["rows"]),
        mesh=mesh,
        in_specs=(split,) * 6 + (P("rows"),),
        out_specs=(P(None, "width"), P(None, "width"), P("width"), P("width")),
        check_vma=False,
    )
```
